16 devices in a mesh: dp: 2 (over z), tp: 8 (over y, x, core).
Axes of the slice: x: 2, y: 2, z: 2, core: 2. Of those that a mesh axis runs over, the one named last changes fastest.
Arguments:
- act_in: bfloat16 [16, 512, 5120], P('dp'), parts along dimension 0
- ln_gain: float32 [2, 5120], replicated
- ln_bias: float32 [2, 5120], replicated
- w_qkv: bfloat16 [2, 5120, 40, 384], P(None, None, 'tp')
- w_out: bfloat16 [2, 5120, 5120], P(None, 'tp')
- w_up: bfloat16 [2, 5120, 20480], P(None, None, 'tp')
- w_down: bfloat16 [2, 20480, 5120], P(None, 'tp')
Outputs:
- output: bfloat16 [16, 512, 5120], P('dp'), parts along dimension 0
There are 2 independent parts. The reference program is written for one: setup_inputs(seed, part) draws one part's arguments, and reference() takes and returns one part's arrays. A program takes and returns all parts, laid end to end along the dimension named above; an argument that names none is the same for every part.
All inputs are finite; a program needn't handle non-finite values.
Results may differ from the reference program's by a relative error of at most 0.0169081.
Values are sent between devices in bfloat16 or wider.
A program may use at most 1 GiB of HBM per device.

```python
import math
import jax
import jax.numpy as jnp
from jax import lax

D_MODEL = 5120
HEADS = 40
KV_HEADS = 40
HEAD_DIM = 128
FF_DIM = 20480
BATCH = 8
SEQ_LEN = 512
LAYERS = 2

GROUP_HEADS = HEADS // KV_HEADS
LN_EPS = 1e-5
ROPE_BASE = 10000.0
QUERY_GAIN = 2.0


def setup_inputs(seed: int = 0, part: int = 0) -> dict:
    base_key = jax.random.key(seed)
    part_key = jax.random.fold_in(base_key, part)
    key_list = jax.random.split(base_key, 6)
    group_cols = (GROUP_HEADS + 2) * HEAD_DIM
    col_gain = jnp.where(jnp.arange(group_cols) < GROUP_HEADS * HEAD_DIM, QUERY_GAIN, 1.0)
    act_in = jax.random.normal(part_key, (BATCH, SEQ_LEN, D_MODEL), jnp.float32)
    ln_gain = 1.0 + 0.2 * jax.random.normal(key_list[0], (LAYERS, D_MODEL), jnp.float32)
    ln_bias = 0.3 * jax.random.normal(key_list[1], (LAYERS, D_MODEL), jnp.float32)
    w_qkv = jax.random.normal(key_list[2], (LAYERS, D_MODEL, KV_HEADS, group_cols), jnp.float32) * col_gain * D_MODEL ** -0.5
    w_out = jax.random.normal(key_list[3], (LAYERS, HEADS * HEAD_DIM, D_MODEL), jnp.float32) * (1.5 * (HEADS * HEAD_DIM) ** -0.5)
    w_up = jax.random.normal(key_list[4], (LAYERS, D_MODEL, FF_DIM), jnp.float32) * D_MODEL ** -0.5
    w_down = jax.random.normal(key_list[5], (LAYERS, FF_DIM, D_MODEL), jnp.float32) * FF_DIM ** -0.5
    return {"act_in": act_in.astype(jnp.bfloat16), "ln_gain": ln_gain, "ln_bias": ln_bias, "w_qkv": w_qkv.astype(jnp.bfloat16), "w_out": w_out.astype(jnp.bfloat16), "w_up": w_up.astype(jnp.bfloat16), "w_down": w_down.astype(jnp.bfloat16)}


def layer_norm(hidden, gain, bias):
    hidden_f = hidden.astype(jnp.float32)
    row_mean = jnp.mean(hidden_f, axis=-1, keepdims=True)
    centered = hidden_f - row_mean
    row_var = jnp.mean(centered * centered, axis=-1, keepdims=True)
    return (centered * lax.rsqrt(row_var + LN_EPS) * gain + bias).astype(jnp.bfloat16)


def rope_tables():
    half_dim = HEAD_DIM // 2
    inv_freq = ROPE_BASE ** (-2.0 * jnp.arange(half_dim, dtype=jnp.float32) / HEAD_DIM)
    angles = jnp.arange(SEQ_LEN, dtype=jnp.float32)[:, None] * inv_freq[None, :]
    return jnp.cos(angles), jnp.sin(angles)


def apply_rope(proj, cos_tab, sin_tab):
    half_dim = proj.shape[-1] // 2
    first = proj[..., :half_dim]
    second = proj[..., half_dim:]
    return jnp.concatenate([first * cos_tab - second * sin_tab, second * cos_tab + first * sin_tab], axis=-1)


def attend_sequence(operands):
    query, keys, values = operands
    scores = jnp.einsum("sgrd,tgd->grst", query.astype(jnp.float32), keys.astype(jnp.float32)) / math.sqrt(HEAD_DIM)
    positions = jnp.arange(SEQ_LEN)
    allowed = positions[:, None] >= positions[None, :]
    scores = jnp.where(allowed, scores, -1e30)
    attn_probs = jax.nn.softmax(scores, axis=-1).astype(jnp.bfloat16)
    context = jnp.einsum("grst,tgd->sgrd", attn_probs.astype(jnp.float32), values.astype(jnp.float32))
    return context.astype(jnp.bfloat16)


def layer_step(hidden, params):
    gain, bias, w_qkv, w_out, w_up, w_down = params
    normed = layer_norm(hidden, gain, bias)
    flat = normed.reshape(BATCH * SEQ_LEN, D_MODEL)
    qkv_proj = jnp.dot(flat, w_qkv.reshape(D_MODEL, -1), preferred_element_type=jnp.float32)
    qkv_proj = qkv_proj.reshape(BATCH, SEQ_LEN, KV_HEADS, GROUP_HEADS + 2, HEAD_DIM)
    cos_tab, sin_tab = rope_tables()
    query = apply_rope(qkv_proj[:, :, :, :GROUP_HEADS], cos_tab[None, :, None, None, :], sin_tab[None, :, None, None, :]).astype(jnp.bfloat16)
    keys = apply_rope(qkv_proj[:, :, :, GROUP_HEADS], cos_tab[None, :, None, :], sin_tab[None, :, None, :]).astype(jnp.bfloat16)
    values = qkv_proj[:, :, :, GROUP_HEADS + 1].astype(jnp.bfloat16)
    context = lax.map(attend_sequence, (query, keys, values))
    attn_part = jnp.dot(context.reshape(BATCH * SEQ_LEN, HEADS * HEAD_DIM), w_out, preferred_element_type=jnp.float32)
    up_proj = jnp.dot(flat, w_up, preferred_element_type=jnp.float32)
    gelu_out = jax.nn.gelu(up_proj, approximate=False).astype(jnp.bfloat16)
    mlp_part = jnp.dot(gelu_out, w_down, preferred_element_type=jnp.float32)
    update = (attn_part + mlp_part).astype(jnp.bfloat16).reshape(BATCH, SEQ_LEN, D_MODEL)
    new_hidden = (hidden.astype(jnp.float32) + update.astype(jnp.float32)).astype(jnp.bfloat16)
    return new_hidden, None


def reference(act_in, ln_gain, ln_bias, w_qkv, w_out, w_up, w_down):
    act_out = lax.scan(layer_step, act_in, (ln_gain, ln_bias, w_qkv, w_out, w_up, w_down))[0]
    return act_out
```

```python
import functools

import jax
import jax.numpy as jnp
from jax import lax
from jax.experimental import pallas as pl
from jax.experimental.pallas import tpu as pltpu
from jax.sharding import PartitionSpec as P

LN_EPS = 1e-5
ROPE_BASE = 10000.0
HEAD = 128
TILE = 512
F32 = jnp.float32
BF16 = jnp.bfloat16
VMEM_LIMIT = 66_500_000
COMM = True


def layer_norm(rows, gain, bias):
    rows = rows.astype(F32)
    centered = rows - jnp.mean(rows, axis=-1, keepdims=True)
    row_var = jnp.mean(centered * centered, axis=-1, keepdims=True)
    return (centered * lax.rsqrt(row_var + LN_EPS) * gain + bias).astype(BF16)


def gelu(val):
    return 0.5 * val * (1.0 + lax.erf(val * (0.5 ** 0.5)))


def rope_tables(seq_len):
    half = HEAD // 2
    inv_freq = ROPE_BASE ** (-2.0 * jnp.arange(half, dtype=F32) / HEAD)
    angles = jnp.arange(seq_len, dtype=F32)[:, None] * inv_freq[None, :]
    cos, sin = jnp.cos(angles), jnp.sin(angles)
    ones, zeros = jnp.ones((seq_len, HEAD), F32), jnp.zeros((seq_len, HEAD), F32)
    cos_tab = jnp.stack([jnp.concatenate([cos, cos], -1), ones])
    sin_tab = jnp.stack([jnp.concatenate([-sin, sin], -1), zeros])
    return cos_tab, sin_tab


def head_context(query, keys, values, scale):
    scores = lax.dot_general(query, keys, (((1,), (1,)), ((), ())), preferred_element_type=F32)
    rows, cols = scores.shape
    row_ids = lax.broadcasted_iota(jnp.int32, (rows, cols), 0) + (cols - rows)
    col_ids = lax.broadcasted_iota(jnp.int32, (rows, cols), 1)
    scores = jnp.where(row_ids >= col_ids, scores, -1e30)
    top = jnp.max(scores, axis=-1, keepdims=True)
    weights = jnp.exp((scores - top) * scale)
    probs = weights * (1.0 / jnp.sum(weights, axis=-1, keepdims=True))
    return jnp.dot(probs.astype(BF16), values, preferred_element_type=F32).astype(BF16)


def mega_kernel(seqs, heads, x_hbm, gain_ref, bias_ref, cos_ref, sin_ref, wq_hbm, wo_hbm, wu_hbm, wd_hbm, g_hbm,
                norm, w_a, w_b, mid, qkv, part, pair, rs1, rs2, resid, shard,
                sem_a, sem_b, sem_x, sem_pair_s, sem_pair_r, sem_res, sem_loc,
                rs1_s, rs1_r, rs2_s, rs2_r, ag1_s, ag1_r, ag2_s, ag2_r, fin_s, fin_r):
    layers = wq_hbm.shape[0]
    d_model = wq_hbm.shape[2]
    seq_len = x_hbm.shape[1]
    steps = layers * seqs
    q_blocks = 3 * heads
    q_tiles = (q_blocks * HEAD + TILE - 1) // TILE
    attn_width = heads * HEAD
    ups = heads
    downs = 5
    t_down = d_model // downs
    half = seq_len // 2
    sub = half // 2
    q32 = sub // 4
    q16 = sub // 8
    ln_rows = seq_len // (downs - 1)
    scale = HEAD ** -0.5

    me = lax.axis_index("tp")
    core = me % 2
    x_pos = (me // 2) % 2
    y_pos = me // 4
    partner = me + 1 - 2 * core
    x_nbr = me + 2 - 4 * x_pos
    y_nbr = me + 4 - 8 * y_pos

    def remote(src, dst, s_sem, r_sem, target):
        return pltpu.make_async_remote_copy(src_ref=src, dst_ref=dst, send_sem=s_sem, recv_sem=r_sem,
                                            device_id={"tp": target}, device_id_type=pl.DeviceIdType.MESH)

    local = pltpu.make_async_copy

    def start_q(layer, tile, slot):
        for k in range(TILE // HEAD):
            blk = jnp.minimum(tile * (TILE // HEAD) + k, q_blocks - 1)
            col = pl.multiple_of((blk % 3) * HEAD, HEAD)
            local(wq_hbm.at[layer, blk // 3, :, pl.ds(col, HEAD)], w_a.at[slot, :, pl.ds(k * HEAD, HEAD)], sem_a.at[slot]).start()

    def start_u(layer, tile, slot):
        col = pl.multiple_of(tile * TILE, TILE)
        local(wu_hbm.at[layer, :, pl.ds(col, TILE)], w_a.at[slot], sem_a.at[slot]).start()

    def wait_a(slot):
        local(wu_hbm.at[0, :, pl.ds(0, TILE)], w_a.at[slot], sem_a.at[slot]).wait()

    def start_b(layer, tile, slot):
        col = pl.multiple_of(tile * t_down, t_down)
        local(wo_hbm.at[layer, :, pl.ds(col, t_down)], w_b.at[slot, pl.ds(0, attn_width)], sem_b.at[slot, 0]).start()
        local(wd_hbm.at[layer, :, pl.ds(col, t_down)], w_b.at[slot, pl.ds(attn_width, wd_hbm.shape[1])], sem_b.at[slot, 1]).start()

    def wait_b(slot):
        local(wo_hbm.at[0, :, pl.ds(0, t_down)], w_b.at[slot, pl.ds(0, attn_width)], sem_b.at[slot, 0]).wait()
        local(wd_hbm.at[0, :, pl.ds(0, t_down)], w_b.at[slot, pl.ds(attn_width, wd_hbm.shape[1])], sem_b.at[slot, 1]).wait()

    def start_x(step):
        @pl.when(step < seqs)
        def _():
            local(x_hbm.at[step], norm.at[pl.ds(0, seq_len)], sem_x).start()

        @pl.when(step >= seqs)
        def _():
            local(g_hbm.at[jnp.maximum(step - seqs, 0)], norm.at[pl.ds(0, seq_len)], sem_x).start()

    def wait_x():
        local(x_hbm.at[0], norm.at[pl.ds(0, seq_len)], sem_x).wait()

    def norm_block(layer, blk):
        rows = pl.ds(pl.multiple_of(blk * ln_rows, ln_rows), ln_rows)
        norm[rows, :] = layer_norm(norm[rows, :], gain_ref[layer], bias_ref[layer])

    base = core * half

    def keep32(u, colour):
        pos = x_pos if colour == 0 else y_pos
        return u * sub + colour * (sub // 2) + pos * q32

    def send32(u, colour):
        pos = x_pos if colour == 0 else y_pos
        return u * sub + colour * (sub // 2) + (1 - pos) * q32

    def keep16(u, colour):
        pos = y_pos if colour == 0 else x_pos
        return keep32(u, colour) + pos * q16

    def send16(u, colour):
        pos = y_pos if colour == 0 else x_pos
        return keep32(u, colour) + (1 - pos) * q16

    first_nbr = (x_nbr, y_nbr)
    second_nbr = (y_nbr, x_nbr)

    def al(val):
        return pl.multiple_of(val, q16)

    def pair_copy(slot, tile):
        cols = pl.ds(pl.multiple_of(tile * t_down, t_down), t_down)
        src = part.at[pl.ds(pl.multiple_of((1 - core) * half, half), half), cols]
        return remote(src, pair.at[slot, :, cols], sem_pair_s.at[slot], sem_pair_r.at[slot], partner)

    def rs1_copy(slot, u, k):
        return remote(pair.at[slot, pl.ds(al(send32(u, k)), q32)], rs1.at[u, k], rs1_s.at[u, k], rs1_r.at[u, k], first_nbr[k])

    def rs2_copy(slot, u, k):
        return remote(pair.at[slot, pl.ds(al(send16(u, k)), q16)], rs2.at[u, k], rs2_s.at[u, k], rs2_r.at[u, k], second_nbr[k])

    def g_rows(seq, start, size):
        return g_hbm.at[seq, pl.ds(al(base + start), size)]

    def ag1_copy(seq, u, k):
        return remote(shard.at[u, k], g_rows(seq, keep16(u, k), q16), ag1_s.at[u, k], ag1_r.at[u, k], second_nbr[k])

    def ag2_copy(seq, u, k):
        rows = g_rows(seq, keep32(u, k), q32)
        return remote(rows, rows, ag2_s.at[u, k], ag2_r.at[u, k], first_nbr[k])

    def fin_copy(seq, u):
        rows = g_rows(seq, u * sub, sub)
        return remote(rows, rows, fin_s.at[lax.rem(seq, 2), u], fin_r.at[lax.rem(seq, 2), u], partner)

    def res_copy(src, seq, u, k):
        return local(src.at[seq, pl.ds(al(base + keep16(u, k)), q16)], resid.at[u, k], sem_res.at[u, k])

    def loc_copy(seq, u, k):
        return local(shard.at[u, k], g_rows(seq, keep16(u, k), q16), sem_loc.at[u, k])

    pairs = [(u, k) for u in range(2) for k in range(2)]

    def reduce_pair(seq):
        slot = seq % 2
        whole = part.at[pl.ds(0, half)]
        remote(whole, pair.at[slot], sem_pair_s.at[slot], sem_pair_r.at[slot], partner).wait()

        @pl.loop(0, half // q32)
        def _(i):
            rows = pl.ds(pl.multiple_of(i * q32, q32), q32)
            mine = part[pl.ds(pl.multiple_of(core * half + i * q32, q32), q32), :].astype(F32)
            pair[slot, rows, :] = (mine + pair[slot, rows, :].astype(F32)).astype(BF16)

        for u, k in pairs:
            rs1_copy(slot, u, k).start()

        for u, k in pairs:
            @pl.when(seq < seqs)
            def _():
                res_copy(x_hbm, seq, u, k).start()

            @pl.when(seq >= seqs)
            def _():
                res_copy(g_hbm, jnp.maximum(seq - seqs, 0), u, k).start()

    def reduce_first(seq, u):
        slot = seq % 2
        for k in range(2):
            rs1_copy(slot, u, k).wait()
            rows = pl.ds(al(keep32(u, k)), q32)
            pair[slot, rows, :] = (pair[slot, rows, :].astype(F32) + rs1[u, k].astype(F32)).astype(BF16)
        for k in range(2):
            rs2_copy(slot, u, k).start()

    def reduce_second(seq, u):
        slot = seq % 2
        for k in range(2):
            rs2_copy(slot, u, k).wait()
            res_copy(x_hbm, 0, u, k).wait()
            rows = pl.ds(al(keep16(u, k)), q16)
            update = (pair[slot, rows, :].astype(F32) + rs2[u, k].astype(F32)).astype(BF16)
            shard[u, k] = (resid[u, k].astype(F32) + update.astype(F32)).astype(BF16)
        for k in range(2):
            loc_copy(seq, u, k).start()
            ag1_copy(seq, u, k).start()

    def gather_first(seq, u):
        for k in range(2):
            loc_copy(seq, u, k).wait()
            ag1_copy(seq, u, k).wait()
        for k in range(2):
            ag2_copy(seq, u, k).start()

    def gather_pair(seq, u):
        for k in range(2):
            ag2_copy(seq, u, k).wait()
        fin_copy(seq, u).start()

    def gather_done(seq):
        for u in range(2):
            fin_copy(seq, u).wait()

    if COMM:
        barrier = pltpu.get_barrier_semaphore()
        for nbr in (partner, x_nbr, y_nbr):
            pl.semaphore_signal(barrier, inc=1, device_id={"tp": nbr}, device_id_type=pl.DeviceIdType.MESH)
        pl.semaphore_wait(barrier, 3)
    start_x(0)
    start_q(0, 0, 0)
    start_q(0, 1, 1)
    wait_x()

    @pl.loop(0, downs - 1)
    def _(blk):
        norm_block(0, blk)

    def when_comm(cond):
        if COMM:
            return pl.when(cond)
        return lambda fn: None

    @pl.loop(0, steps)
    def _(step):
        layer = step // seqs
        prev = step - 1
        has_prev = step >= 1

        @pl.loop(0, q_tiles)
        def _(i):
            nxt = lax.rem(i + 2, 3)

            @pl.when(i + 2 < q_tiles)
            def _():
                start_q(layer, i + 2, nxt)

            @pl.when(i + 2 >= q_tiles)
            def _():
                start_u(layer, i + 2 - q_tiles, nxt)

            slot = lax.rem(i, 3)
            wait_a(slot)
            prod = jnp.dot(norm[pl.ds(0, seq_len), :], w_a[slot], preferred_element_type=F32)
            for k in range(TILE // HEAD):
                blk = prod[:, k * HEAD:(k + 1) * HEAD]
                kind = (i * (TILE // HEAD) + k) % 3 // 2
                turned = blk * cos_ref[kind] + pltpu.roll(blk, HEAD // 2, 1) * sin_ref[kind]
                col = pl.multiple_of(i * TILE + k * HEAD, HEAD)
                qkv[:, pl.ds(col, HEAD)] = turned.astype(BF16)

            @when_comm((i == 0) & has_prev)
            def _():
                reduce_pair(prev)

            @when_comm((i == 1) & (step >= 2))
            def _():
                gather_pair(prev - 1, 1)

            @when_comm((i == 3) & (step >= 2))
            def _():
                gather_done(prev - 1)

            @when_comm((i == 3) & has_prev)
            def _():
                reduce_first(prev, 0)

        start_b(layer, 0, lax.rem(step * downs, 2))

        @pl.loop(0, ups)
        def _(j):
            a = q_tiles + j
            nxt = lax.rem(a + 2, 3)

            @pl.when(j + 2 < ups)
            def _():
                start_u(layer, j + 2, nxt)

            @pl.when((j + 2 >= ups) & (step + 1 < steps))
            def _():
                start_q((step + 1) // seqs, j + 2 - ups, nxt)

            slot = lax.rem(a, 3)
            wait_a(slot)
            prod = jnp.dot(norm[pl.ds(0, seq_len), :], w_a[slot], preferred_element_type=F32)
            mid[:, pl.ds(pl.multiple_of(attn_width + j * TILE, HEAD), TILE)] = gelu(prod).astype(BF16)
            q_cols = pl.ds(pl.multiple_of(j * 3 * HEAD, HEAD), HEAD)
            k_cols = pl.ds(pl.multiple_of(j * 3 * HEAD + HEAD, HEAD), HEAD)
            v_cols = pl.ds(pl.multiple_of(j * 3 * HEAD + 2 * HEAD, HEAD), HEAD)
            o_cols = pl.ds(pl.multiple_of(j * HEAD, HEAD), HEAD)
            for blk in range(2):
                rows = pl.ds(blk * half, half)
                seen = pl.ds(0, (blk + 1) * half)
                mid[rows, o_cols] = head_context(qkv[rows, q_cols], qkv[seen, k_cols], qkv[seen, v_cols], scale)

            @when_comm((j == 1) & has_prev)
            def _():
                reduce_first(prev, 1)

            @when_comm((j == 3) & has_prev)
            def _():
                reduce_second(prev, 0)

            @when_comm((j == 4) & has_prev)
            def _():
                reduce_second(prev, 1)

        @pl.loop(0, downs)
        def _(j):
            slot = lax.rem(step * downs + j, 2)

            @pl.when(j + 1 < downs)
            def _():
                start_b(layer, j + 1, 1 - slot)

            @pl.when((j == 0) & (step + 1 < steps))
            def _():
                start_x(step + 1)

            @pl.when((j == 1) & (step + 1 < steps))
            def _():
                wait_x()

            wait_b(slot)
            prod = jnp.dot(mid[...], w_b[slot], preferred_element_type=F32)
            part[:, pl.ds(pl.multiple_of(j * t_down, t_down), t_down)] = prod.astype(BF16)
            norm_block(jnp.minimum((step + 1) // seqs, layers - 1), (j + downs - 1) % downs)
            if COMM:
                pair_copy(lax.rem(step, 2), j).start()

            @when_comm((j == 0) & has_prev)
            def _():
                gather_first(prev, 0)

            @when_comm((j == 1) & has_prev)
            def _():
                gather_first(prev, 1)

            @when_comm((j == 3) & has_prev)
            def _():
                gather_pair(prev, 0)

    if COMM:
        last = steps - 1
        reduce_pair(last)
        gather_pair(last - 1, 1)
        gather_done(last - 1)
        for u in range(2):
            reduce_first(last, u)
        for u in range(2):
            reduce_second(last, u)
        for u in range(2):
            gather_first(last, u)
        for u in range(2):
            gather_pair(last, u)
        gather_done(last)
    else:
        cp = local(part, g_hbm.at[0], sem_x)
        cp.start()
        cp.wait()


def mega_call(x, gain, bias, w_qkv, w_out, w_up, w_down):
    seqs, seq_len, d_model = x.shape
    layers, _, heads, _ = w_qkv.shape
    w_q = jnp.transpose(w_qkv, (0, 2, 1, 3))
    cos_tab, sin_tab = rope_tables(seq_len)
    mid_width = heads * HEAD + w_down.shape[1]
    half = seq_len // 2
    sub = half // 2
    t_down = d_model // 5
    q_cols = -(-3 * heads * HEAD // TILE) * TILE
    any_spec = pl.BlockSpec(memory_space=pl.ANY)
    vmem_spec = pl.BlockSpec(memory_space=pltpu.VMEM)
    dma = pltpu.SemaphoreType.DMA
    flops = 2 * layers * seqs * seq_len * d_model * (3 * heads * HEAD + w_up.shape[2] + mid_width)
    return pl.pallas_call(
        functools.partial(mega_kernel, seqs, heads),
        out_shape=jax.ShapeDtypeStruct((layers * seqs, seq_len, d_model), BF16),
        in_specs=[any_spec, vmem_spec, vmem_spec, vmem_spec, vmem_spec, any_spec, any_spec, any_spec, any_spec],
        out_specs=any_spec,
        scratch_shapes=[
            pltpu.VMEM((seq_len + seq_len // 4, d_model), BF16),
            pltpu.VMEM((3, d_model, TILE), BF16),
            pltpu.VMEM((2, mid_width, t_down), BF16),
            pltpu.VMEM((seq_len, mid_width), BF16),
            pltpu.VMEM((seq_len, q_cols), BF16),
            pltpu.VMEM((seq_len, d_model), BF16),
            pltpu.VMEM((2, half, d_model), BF16),
            pltpu.VMEM((2, 2, sub // 4, d_model), BF16),
            pltpu.VMEM((2, 2, sub // 8, d_model), BF16),
            pltpu.VMEM((2, 2, sub // 8, d_model), BF16),
            pltpu.VMEM((2, 2, sub // 8, d_model), BF16),
            dma((3,)), dma((2, 2)), dma, dma((2,)), dma((2,)), dma((2, 2)), dma((2, 2)),
            dma((2, 2)), dma((2, 2)), dma((2, 2)), dma((2, 2)),
            dma((2, 2)), dma((2, 2)), dma((2, 2)), dma((2, 2)), dma((2, 2)), dma((2, 2)),
        ],
        compiler_params=pltpu.CompilerParams(collective_id=0 if COMM else None, has_side_effects=True, vmem_limit_bytes=VMEM_LIMIT),
        cost_estimate=pl.CostEstimate(flops=flops, bytes_accessed=flops // 500, transcendentals=0),
        name="layers",
    )(x, gain[:, None, :], bias[:, None, :], cos_tab, sin_tab, w_q, w_out, w_up, w_down)


def solution(mesh):
    def shard_body(x, gain, bias, w_qkv, w_out, w_up, w_down):
        gathered = mega_call(x, gain, bias, w_qkv, w_out, w_up, w_down)
        return gathered[gathered.shape[0] - x.shape[0]:]

    return jax.shard_map(shard_body, mesh=mesh, in_specs=(P("dp", None, None), P(None, None), P(None, None), P(None, None, "tp", None), P(None, "tp", None), P(None, None, "tp"), P(None, "tp", None)), out_specs=P("dp", None, None), check_vma=False)
```
